128 devices in a mesh: row: 8 (over z, core), col: 16 (over x, y).
Axes of the slice: x: 4, y: 4, z: 4, core: 2. Of those that a mesh axis runs over, the one named last changes fastest.
Arguments:
- tiles: bfloat16 [8, 16, 128, 128, 128], P('row', 'col'), may hold values from -6 to 6
- tile_row: int32 [8, 16, 128], P('row', 'col'), may hold values from 0 to 127, as said below
- tile_col: int32 [8, 16, 128], P('row', 'col'), may hold values from 0 to 63
- tile_count: int32 [8, 16], P('row', 'col'), may hold values from 16 to 128, as said below
- query_ids: int32 [128], replicated, may hold values from 0 to 131071
- damping: float32 [128], replicated, may hold values from 0.006629126 to 0.026516505
Outputs:
- scores: float32 [131072, 128], P(('row', 'col'))
The draws below stay inside these ranges and needn't reach their ends.
Inputs may be any that keep to these rules, and one draw needn't show every extreme that they name: `tile_count`: some device holds exactly 128 live slots; slots at or past the count hold arbitrary finite values and are ignored. `tile_row`: positions may repeat within a device; such tiles add. For every device and every col index o, the live slots name at most 4 distinct values among o * 8 to o * 8 + 7, and every device reaches 4 for some o. `query_ids`: ids may repeat.
All inputs are finite; a program needn't handle non-finite values.
Results may differ from the reference program's by a relative error of at most 0.003.
Values may be sent and summed in bfloat16 or wider, within the bound.
A program may use at most 128 MiB of HBM per device.

```python
import math
import jax
import jax.numpy as jnp
from jax import lax

TILE = 128
BPD = 8
TILES_DEV = 128
QUERIES = 128
TERMS = 4
TOUCH = 4
NBLK = 1024
NODES = 131072
N_ROW = 8
N_COL = 16


def draw_tile_count(key, part):
    shifts = jax.random.randint(key, (N_ROW * N_COL,), 0, 4)
    counts = jnp.right_shift(jnp.full((N_ROW * N_COL,), TILES_DEV, jnp.int32), shifts.astype(jnp.int32))
    fullest = jax.random.randint(jax.random.fold_in(key, 7), (), 0, N_ROW * N_COL)
    counts = counts.at[fullest].set(TILES_DEV)
    return counts.reshape(N_ROW, N_COL).astype(jnp.int32)


def draw_tile_row(key, part):
    devs = N_ROW * N_COL
    owners = jax.random.randint(jax.random.fold_in(key, 11), (devs, TILES_DEV), 0, N_COL)
    starts = jax.random.randint(jax.random.fold_in(key, 12), (devs, N_COL), 0, BPD)
    offsets = jax.random.randint(jax.random.fold_in(key, 13), (devs, TILES_DEV), 0, TOUCH)
    favoured = jax.random.randint(jax.random.fold_in(key, 14), (devs,), 0, N_COL)
    slot = jnp.arange(TILES_DEV, dtype=jnp.int32)
    first = slot < TOUCH
    owners = jnp.where(first[None, :], favoured[:, None], owners)
    offsets = jnp.where(first[None, :], slot[None, :], offsets)
    chosen = jnp.take_along_axis(starts, owners, axis=1)
    local = (chosen + offsets) % BPD
    return (owners * BPD + local).reshape(N_ROW, N_COL, TILES_DEV).astype(jnp.int32)


def with_ends(array, stream_key, low, top_value):
    longest = array.shape.index(max(array.shape))
    spots = []
    for shift in (0, 1):
        where = [jax.random.randint(jax.random.fold_in(stream_key, axis), (), 0, length) for axis, length in enumerate(array.shape)]
        where[longest] = (where[longest] + shift) % array.shape[longest]
        spots.append(tuple(where))
    return array.at[spots[0]].set(low).at[spots[1]].set(top_value)


def levels(key, extent, pieces, least, largest):
    loudness, own = 1.0, jax.random.fold_in(key, 6)
    for dim, shards_of in pieces:
        steps = jnp.exp(jax.random.uniform(jax.random.fold_in(own, dim), (shards_of,), jnp.float32, least / len(pieces), largest / len(pieces)))
        loudness = loudness * jnp.repeat(steps, extent[dim] // shards_of).reshape([-1 if axis == dim else 1 for axis in range(len(extent))])
    return loudness


def normal_values(key, extent, scale, bound, cuts=(), kind=jnp.bfloat16):
    entries = scale * jax.random.normal(key, extent, jnp.float32)
    if cuts:
        entries = entries * levels(key, extent, cuts, -0.22, 0.18)
    return jnp.clip(entries, -bound, bound).astype(kind)


def setup_inputs(seed: int = 0) -> dict:
    keys = jax.random.split(jax.random.key(seed), 7)
    return {
        "tiles": normal_values(keys[0], (N_ROW, N_COL, TILES_DEV, TILE, TILE), 1.0, 6.0, ((0, 8), (1, 16))),
        "tile_row": draw_tile_row(jax.random.fold_in(keys[6], 71), 0),
        "tile_col": with_ends(jax.random.randint(keys[2], (N_ROW, N_COL, TILES_DEV), 0, BPD * N_ROW), jax.random.fold_in(keys[2], 1), 0, (BPD * N_ROW) - 1).astype(jnp.int32),
        "tile_count": draw_tile_count(jax.random.fold_in(keys[6], 71), 0),
        "query_ids": with_ends(jax.random.randint(keys[4], (QUERIES,), 0, NODES), jax.random.fold_in(keys[4], 1), 0, NODES - 1).astype(jnp.int32),
        "damping": jnp.clip(jnp.exp(jax.random.uniform(keys[5], (QUERIES,), jnp.float32, math.log(0.006629126), math.log(0.026516505))), 0.006629126, 0.026516505),
    }


def device_partial(tile_block, rows, cols, count, xcol):
    picked = xcol[cols]
    prod = jnp.einsum("tab,tbq->taq", tile_block.astype(jnp.float32), picked.astype(jnp.float32))
    live = (jnp.arange(tile_block.shape[0], dtype=jnp.int32) < count).astype(jnp.float32)
    prod = prod * live[:, None, None]
    return jax.ops.segment_sum(prod, rows, num_segments=BPD * N_COL)


def reference(tiles, tile_row, tile_col, tile_count, query_ids, damping):
    nodes = NBLK * TILE
    queries = query_ids.shape[0]
    node_ids = jnp.arange(nodes, dtype=jnp.int32)
    xvec = (node_ids[:, None] == query_ids[None, :]).astype(jnp.bfloat16)
    scores = jnp.zeros((nodes, queries), jnp.float32)
    coef = jnp.ones((queries,), jnp.float32)
    for step in range(TERMS):
        xgrid = xvec.reshape(N_ROW, N_COL, BPD, TILE, queries)

        def one_row(ridx):
            def add_col(cidx, total):
                xcol = lax.dynamic_index_in_dim(xgrid, cidx, 1, keepdims=False)
                xcol = xcol.reshape(N_ROW * BPD, TILE, queries)
                tblock = tiles[ridx, cidx]
                part = device_partial(tblock, tile_row[ridx, cidx], tile_col[ridx, cidx], tile_count[ridx, cidx], xcol)
                rounded = lax.optimization_barrier(part.astype(jnp.bfloat16))
                return total + rounded.astype(jnp.float32)

            start = jnp.zeros((BPD * N_COL, TILE, queries), jnp.float32)
            return lax.fori_loop(0, N_COL, add_col, start)

        ysum = lax.map(one_row, jnp.arange(N_ROW, dtype=jnp.int32))
        ysum = ysum.reshape(nodes, queries)
        scores = scores + coef[None, :] * ysum
        coef = coef * damping
        xvec = ysum.astype(jnp.bfloat16)
    return scores
```

```python
import functools

import jax
import jax.numpy as jnp
from jax import lax
from jax.experimental import pallas as pl
from jax.experimental.pallas import tpu as pltpu
from jax.sharding import PartitionSpec as P

TERMS = 4
CHUNKS = 4
ROWS = 128 // CHUNKS
HALF = ROWS // 2
SLOTS = 128
NONE = 128
EMPTY = 48
UNROLL = 16
PERM, SCOL, KEEP, DEND, PKEND, SBASE, JIDX = range(7)
MESH = pl.DeviceIdType.MESH
BF16, F32, I32 = jnp.bfloat16, jnp.float32, jnp.int32


def down(row):
    return jnp.transpose(jnp.broadcast_to(row, (128, 128)))


def slot_tables(rows, cols, count, col_index):
    lane = lax.broadcasted_iota(I32, (128, 128), 1)
    sub = lax.broadcasted_iota(I32, (128, 128), 0)
    lane1 = lax.broadcasted_iota(I32, (1, 128), 1)
    key = jnp.where(lane1 < count, rows, 128)
    key_row = jnp.broadcast_to(key, (128, 128))
    key_col = down(key)

    def total(mask, value=1):
        return jnp.sum(jnp.where(mask, value, 0), axis=0, keepdims=True)

    earlier = (key_col == key_row) & (sub < lane)
    rank = total((key_col < key_row) | earlier)
    repeat = jnp.minimum(total(earlier), 1)
    place = down(rank) == lane
    perm = total(place, sub)
    scol = total(place, down(cols))
    keep = total(place, down(repeat))
    touched = total(key_col == lane) > 0
    upto = total(key_col <= lane)
    dend = jnp.where(touched, upto - 1, NONE)
    touched_col = down(touched.astype(I32)) > 0
    before = total(touched_col & ((sub >> 3) == (lane >> 3)) & (sub < lane))
    jidx = jnp.where(touched, before, 4)
    packed = touched_col & ((sub >> 3) == (lane >> 2)) & (down(before) == (lane & 3))
    ends = total(packed, down(upto))
    pkend = jnp.where(ends > 0, ends - 1, NONE)
    sbase = (((scol >> 3) * 16 + col_index) * 8 + (scol & 7)) * 128
    return jnp.concatenate([perm, scol, keep, dend, pkend, sbase, jidx, jidx], axis=0)


def kernel(tiles_hbm, trow, tcol, count, qids, damping, out, *scratch):
    scratch = list(scratch)
    take = lambda n: [scratch.pop(0) for _ in range(n)]
    raw, flip, tabv, tabs, metav, idxv, idxs, qmat, coef, own, score = take(11)
    run = take(CHUNKS)
    xg = [take(CHUNKS) for _ in range(2)]
    recv1 = [[take(2) for _ in range(CHUNKS)] for _ in range(2)]
    send1, send2, recv2 = take(3)
    tile_sem, copy_sem, meta_ss, meta_rs, ss1, rs1, ss2, rs2, zss, zrs, css, crs = take(12)

    row, col = lax.axis_index("row"), lax.axis_index("col")
    z, core = row // 2, row % 2
    x, y = col // 4, col % 4
    wrap = lambda v, d: (v + d) % 4
    along = (
        lambda d: {"row": row, "col": wrap(x, d) * 4 + y},
        lambda d: {"row": row, "col": x * 4 + wrap(y, d)},
    )
    up = lambda d: {"row": wrap(z, d) * 2 + core, "col": col}
    other = {"row": z * 2 + 1 - core, "col": col}

    load = pltpu.make_async_copy(tiles_hbm, raw, tile_sem)
    load.start()
    barrier = pltpu.get_barrier_semaphore()
    peers = [f(d) for f in (*along, up) for d in (1, 2, 3)] + [other]
    for peer in peers:
        pl.semaphore_signal(barrier, inc=1, device_id=peer, device_id_type=MESH)

    def remote(src, dst, send_sem, recv_sem, peer):
        return pltpu.make_async_remote_copy(
            src_ref=src, dst_ref=dst, send_sem=send_sem, recv_sem=recv_sem, device_id=peer, device_id_type=MESH
        )

    tabv[...] = slot_tables(trow[...], tcol[...], count[0, 0], col)
    to_scalar = pltpu.make_async_copy(tabv, tabs, copy_sem.at[0])
    to_scalar.start()
    lane = lax.broadcasted_iota(I32, (128, 128), 1)
    qmat[...] = down(qids[...]) - lane
    coef[...] = down(damping[...])
    for h in range(CHUNKS):
        run[h][NONE] = jnp.zeros((ROWS, 128), BF16)
        for parity in range(2):
            for half in range(2):
                recv1[parity][h][half][EMPTY] = jnp.zeros((HALF, 128), BF16)
    pl.semaphore_wait(barrier, len(peers))
    meta = []
    for half in range(2):
        for d in (1, 2, 3):
            at = half * 3 + d - 1
            meta.append(remote(tabv, metav.at[at], meta_ss.at[at], meta_rs.at[at], along[half](d)))
            meta[-1].start()
    to_scalar.wait()
    load.wait()

    def first_products():
        def body(step, total):
            for u in range(UNROLL // 2):
                s = step * (UNROLL // 2) + u
                tile = raw[tabs[PERM, s]]
                hot = (qmat[...] == tabs[SBASE, s]).astype(BF16)
                prod = lax.dot_general(hot, tile, (((1,), (1,)), ((), ())), preferred_element_type=F32)
                total = jnp.where(tabs[KEEP, s] > 0, prod + total, prod)
                rounded = total.astype(BF16)
                for h in range(CHUNKS):
                    run[h][s] = rounded[h * ROWS : (h + 1) * ROWS]
                flip[s] = jnp.transpose(tile)
            return total

        lax.fori_loop(0, SLOTS // (UNROLL // 2), body, jnp.zeros((128, 128), F32))

    def products(t, h):
        source = xg[(t - 1) % 2][h]

        def body(step, total):
            for u in range(UNROLL):
                s = step * UNROLL + u
                prod = jnp.dot(source[tabs[SCOL, s]], flip[s], preferred_element_type=F32)
                total = jnp.where(tabs[KEEP, s] > 0, prod + total, prod)
                run[h][s] = total.astype(BF16)
            return total

        lax.fori_loop(0, SLOTS // UNROLL, body, jnp.zeros((ROWS, 128), F32))

    copies = {}

    def step1(t, h, half, d):
        return remote(
            send1.at[h, half, d - 1],
            recv1[t % 2][h][half].at[pl.ds((d - 1) * 16, 16)],
            ss1.at[t % 2, h, half, d - 1],
            rs1.at[t % 2, h, half, d - 1],
            along[half](d),
        )

    def step2(t, h, half, e):
        return remote(
            send2.at[h, half, e - 1],
            recv2.at[t % 2, h, half, e - 1],
            ss2.at[t % 2, h, half, e - 1],
            rs2.at[t % 2, h, half, e - 1],
            along[1 - half](e),
        )

    def ship(t, h):
        def body(d, _):
            for half in range(2):
                rows = pl.ds(half * HALF, HALF)
                for e in range(4):
                    if half == 0:
                        dest = wrap(x, d) * 4 + wrap(y, e)
                    else:
                        dest = wrap(x, e) * 4 + wrap(y, d)
                    for j in range(4):
                        send1[h, half, d - 1, e * 4 + j] = run[h][tabs[PKEND, dest * 4 + j], rows, :]
                step1(t, h, half, d).start()
            return 0

        lax.fori_loop(1, 4, body, 0)

    def merge(t, h):
        for half in range(2):
            for d in (1, 2, 3):
                step1(t, h, half, d).wait()
            rows = pl.ds(half * HALF, HALF)
            got = recv1[t % 2][h][half]

            def summed(e, b):
                dest = x * 4 + wrap(y, e) if half == 0 else wrap(x, e) * 4 + y
                block = dest * 8 + b
                total = run[h][tabs[DEND, block], rows, :].astype(F32)
                for d in (1, 2, 3):
                    total = total + got[idxs[half * 3 + d - 1, block]].astype(F32)
                return total

            def body(e, _):
                for b in range(8):
                    send2[h, half, e - 1, b] = summed(e, b).astype(BF16)
                step2(t, h, half, e).start()
                return 0

            lax.fori_loop(1, 4, body, 0)

            def body_own(b, _):
                own[h, half, b] = summed(0, b)
                return 0

            lax.fori_loop(0, 8, body_own, 0)

    def finish(t, h):
        for half in range(2):
            for e in (1, 2, 3):
                step2(t, h, half, e).wait()
        base = pl.multiple_of(row * 8, 8)
        factors = []
        for half in range(2):
            queries = pl.ds(h * ROWS + half * HALF, HALF)
            factor = coef[queries, :]
            for _ in range(t - 1):
                factor = factor * coef[queries, :]
            factors.append(factor)

        def body(b, _):
            for half in range(2):
                queries = pl.ds(h * ROWS + half * HALF, HALF)
                total = own[h, half, b]
                for e in range(3):
                    total = total + recv2[t % 2, h, half, e, b].astype(F32)
                if t == 0:
                    score[b, queries, :] = total
                else:
                    score[b, queries, :] = score[b, queries, :] + factors[half] * total
                if t + 1 < TERMS:
                    xg[t % 2][h][base + b, pl.ds(half * HALF, HALF), :] = total.astype(BF16)
            return 0

        lax.fori_loop(0, 8, body, 0)
        if t + 1 < TERMS:
            mine = xg[t % 2][h].at[pl.ds(base, 8)]
            for d in (1, 2, 3):
                c = remote(mine, mine, zss.at[t % 2, h, d - 1], zrs.at[t % 2, h, d - 1], up(d))
                c.start()
                copies[3, t, h, d] = c
            c = remote(mine, mine, css.at[t % 2, h, 0], crs.at[t % 2, h, 0], other)
            c.start()
            copies[4, t, h, 0] = c

    def hand_on(t, h):
        for d in (1, 3, 2):
            copies[3, t, h, d].wait()
            source = pl.multiple_of((wrap(z, 4 - d) * 2 + core) * 8, 8)
            part = xg[t % 2][h].at[pl.ds(source, 8)]
            c = remote(part, part, css.at[t % 2, h, d], crs.at[t % 2, h, d], other)
            c.start()
            copies[4, t, h, d] = c

    def gathered(t, h):
        for d in range(4):
            copies[4, t, h, d].wait()

    first_products()
    for h in range(CHUNKS):
        ship(0, h)
    for c in meta:
        c.wait()
    lane1 = lax.broadcasted_iota(I32, (1, 128), 1)
    for half in range(2):
        for d in (1, 2, 3):
            place = metav[half * 3 + d - 1, JIDX : JIDX + 1, :]
            away = (((lane1 >> 3) & 3) - y + 4) & 3 if half == 0 else ((lane1 >> 5) - x + 4) & 3
            idxv[half * 3 + d - 1 : half * 3 + d, :] = jnp.where(place < 4, (d - 1) * 16 + away * 4 + place, EMPTY)
    idxv[6:8, :] = jnp.zeros((2, 128), I32)
    to_scalar = pltpu.make_async_copy(idxv, idxs, copy_sem.at[1])
    to_scalar.start()
    to_scalar.wait()
    for t in range(TERMS):
        for h in range(CHUNKS):
            merge(t, h)
        for h in range(CHUNKS):
            finish(t, h)
        if t + 1 < TERMS:
            for h in range(CHUNKS):
                hand_on(t, h)
            for h in range(CHUNKS):
                gathered(t, h)
                products(t + 1, h)
                ship(t + 1, h)
    for b in range(8):
        out[b * 128 : (b + 1) * 128, :] = jnp.transpose(score[b])


def shards(tiles, tile_row, tile_col, tile_count, query_ids, damping):
    vmem = pl.BlockSpec(memory_space=pltpu.VMEM)
    dma = pltpu.SemaphoreType.DMA
    return pl.pallas_call(
        kernel,
        out_shape=jax.ShapeDtypeStruct((1024, 128), F32),
        in_specs=[pl.BlockSpec(memory_space=pl.ANY), vmem, vmem, pl.BlockSpec(memory_space=pltpu.SMEM), vmem, vmem],
        out_specs=vmem,
        scratch_shapes=[
            pltpu.VMEM((SLOTS, 128, 128), BF16),
            pltpu.VMEM((SLOTS, 128, 128), BF16),
            pltpu.VMEM((8, 128), I32),
            pltpu.SMEM((8, 128), I32),
            pltpu.VMEM((6, 8, 128), I32),
            pltpu.VMEM((8, 128), I32),
            pltpu.SMEM((8, 128), I32),
            pltpu.VMEM((128, 128), I32),
            pltpu.VMEM((128, 128), F32),
            pltpu.VMEM((CHUNKS, 2, 8, HALF, 128), F32),
            pltpu.VMEM((8, 128, 128), F32),
            *[pltpu.VMEM((SLOTS + 1, ROWS, 128), BF16) for _ in range(CHUNKS)],
            *[pltpu.VMEM((64, ROWS, 128), BF16) for _ in range(2 * CHUNKS)],
            *[pltpu.VMEM((EMPTY + 1, HALF, 128), BF16) for _ in range(4 * CHUNKS)],
            pltpu.VMEM((CHUNKS, 2, 3, 16, HALF, 128), BF16),
            pltpu.VMEM((CHUNKS, 2, 3, 8, HALF, 128), BF16),
            pltpu.VMEM((2, CHUNKS, 2, 3, 8, HALF, 128), BF16),
            dma,
            dma((2,)),
            dma((6,)),
            dma((6,)),
            dma((2, CHUNKS, 2, 3)),
            dma((2, CHUNKS, 2, 3)),
            dma((2, CHUNKS, 2, 3)),
            dma((2, CHUNKS, 2, 3)),
            dma((2, CHUNKS, 3)),
            dma((2, CHUNKS, 3)),
            dma((2, CHUNKS, 4)),
            dma((2, CHUNKS, 4)),
        ],
        compiler_params=pltpu.CompilerParams(collective_id=0, has_side_effects=True, vmem_limit_bytes=60 * 2**20),
        name="katz",
    )(
        tiles.reshape(SLOTS, 128, 128),
        tile_row.reshape(1, SLOTS),
        tile_col.reshape(1, SLOTS),
        tile_count,
        query_ids.reshape(1, 128),
        damping.reshape(1, 128),
    )


def solution(mesh):
    in_specs = (
        P("row", "col", None, None, None),
        P("row", "col", None),
        P("row", "col", None),
        P("row", "col"),
        P(),
        P(),
    )
    out_specs = P(("row", "col"), None)
    return jax.shard_map(shards, mesh=mesh, in_specs=in_specs, out_specs=out_specs, check_vma=False)
```

```python
import functools

import jax
import jax.numpy as jnp
from jax import lax
from jax.experimental import pallas as pl
from jax.experimental.pallas import tpu as pltpu
from jax.sharding import PartitionSpec as P

TERMS = 4
GROUP = 2
CHUNKS = 8
ROWS = 128 // CHUNKS
SLOTS = 128
NONE = 128
EMPTY = 48
UNROLL = 64
FIRST = 1
MERGE, FINISH, HAND_ON, NEXT = 0.28, 0.55, 0.85, 0.99
LATER, SPREAD = 0.06, 1.0
PERM, SCOL, KEEP, DEND, PKEND, SBASE, JIDX = range(7)
MESH = pl.DeviceIdType.MESH
BF16, F32, I32 = jnp.bfloat16, jnp.float32, jnp.int32


def down(row):
    return jnp.transpose(jnp.broadcast_to(row, (128, 128)))


def slot_tables(rows, cols, count, col_index):
    lane = lax.broadcasted_iota(I32, (128, 128), 1)
    sub = lax.broadcasted_iota(I32, (128, 128), 0)
    lane1 = lax.broadcasted_iota(I32, (1, 128), 1)
    key = jnp.where(lane1 < count, rows, 128)
    key_row = jnp.broadcast_to(key, (128, 128))
    key_col = down(key)

    def total(mask, value=1):
        return jnp.sum(jnp.where(mask, value, 0), axis=0, keepdims=True)

    earlier = (key_col == key_row) & (sub < lane)
    rank = total((key_col < key_row) | earlier)
    repeat = jnp.minimum(total(earlier), 1)
    place = down(rank) == lane
    perm = total(place, sub)
    scol = total(place, down(cols))
    keep = total(place, down(repeat))
    touched = total(key_col == lane) > 0
    upto = total(key_col <= lane)
    dend = jnp.where(touched, upto - 1, NONE)
    touched_col = down(touched.astype(I32)) > 0
    before = total(touched_col & ((sub >> 3) == (lane >> 3)) & (sub < lane))
    jidx = jnp.where(touched, before, 4)
    packed = touched_col & ((sub >> 3) == (lane >> 2)) & (down(before) == (lane & 3))
    ends = total(packed, down(upto))
    pkend = jnp.where(ends > 0, ends - 1, NONE)
    sbase = (((scol >> 3) * 16 + col_index) * 8 + (scol & 7)) * 128
    return jnp.concatenate([perm, scol, keep, dend, pkend, sbase, jidx, jidx], axis=0)


def kernel(tiles_hbm, trow, tcol, count, qids, damping, out, *scratch):
    scratch = list(scratch)
    take = lambda n: [scratch.pop(0) for _ in range(n)]
    raw, flip, tabv, tabs, metav, idxv, idxs, qmat, coef, own, score = take(11)
    run = take(CHUNKS // GROUP)
    xg = [take(CHUNKS) for _ in range(2)]
    recv1 = [take(CHUNKS) for _ in range(2)]
    send1, send2, recv2 = take(3)
    tile_sem, copy_sem, meta_ss, meta_rs, ss1, rs1, ss2, rs2, zss, zrs, css, crs = take(12)

    row, col = lax.axis_index("row"), lax.axis_index("col")
    z, core = row // 2, row % 2
    x, y = col // 4, col % 4
    wrap = lambda v, d: (v + d) % 4
    along = (
        lambda d: {"row": row, "col": wrap(x, d) * 4 + y},
        lambda d: {"row": row, "col": x * 4 + wrap(y, d)},
    )
    up = lambda d: {"row": wrap(z, d) * 2 + core, "col": col}
    other = {"row": z * 2 + 1 - core, "col": col}

    load = pltpu.make_async_copy(tiles_hbm, raw, tile_sem)
    load.start()
    barrier = pltpu.get_barrier_semaphore()
    peers = [f(d) for f in (*along, up) for d in (1, 2, 3)] + [other]
    for peer in peers:
        pl.semaphore_signal(barrier, inc=1, device_id=peer, device_id_type=MESH)

    def remote(src, dst, send_sem, recv_sem, peer):
        return pltpu.make_async_remote_copy(
            src_ref=src, dst_ref=dst, send_sem=send_sem, recv_sem=recv_sem, device_id=peer, device_id_type=MESH
        )

    tabv[...] = slot_tables(trow[...], tcol[...], count[0, 0], col)
    to_scalar = pltpu.make_async_copy(tabv, tabs, copy_sem.at[0])
    to_scalar.start()
    lane = lax.broadcasted_iota(I32, (128, 128), 1)
    qmat[...] = down(qids[...]) - lane
    coef[...] = down(damping[...])
    for g in range(CHUNKS // GROUP):
        run[g][NONE] = jnp.zeros((GROUP * ROWS, 128), BF16)
    for h in range(CHUNKS):
        for parity in range(2):
            recv1[parity][h][EMPTY] = jnp.zeros((ROWS, 128), BF16)
    to_scalar.wait()
    load.wait()

    def first_products():
        def body(step, total):
            for u in range(8):
                s = step * (8) + u
                tile = raw[tabs[PERM, s]]
                hot = (qmat[...] == tabs[SBASE, s]).astype(BF16)
                prod = lax.dot_general(hot, tile, (((1,), (1,)), ((), ())), preferred_element_type=F32)
                total = jnp.where(tabs[KEEP, s] > 0, prod + total, prod)
                rounded = total.astype(BF16)
                for g in range(CHUNKS // GROUP):
                    run[g][s] = rounded[g * GROUP * ROWS : (g + 1) * GROUP * ROWS]
                flip[s] = jnp.transpose(tile)
            return total

        lax.fori_loop(0, SLOTS // (8), body, jnp.zeros((128, 128), F32))

    def products(t, g):
        sources = [xg[(t - 1) % 2][g * GROUP + i] for i in range(GROUP)]

        def body(step, total):
            for u in range(UNROLL):
                s = step * UNROLL + u
                left = jnp.concatenate([source[tabs[SCOL, s]] for source in sources], axis=0)
                prod = jnp.dot(left, flip[s], preferred_element_type=F32)
                total = jnp.where(tabs[KEEP, s] > 0, prod + total, prod)
                run[g][s] = total.astype(BF16)
            return total

        lax.fori_loop(0, SLOTS // UNROLL, body, jnp.zeros((GROUP * ROWS, 128), F32))

    def part(h, index):
        return run[h // GROUP][index, pl.ds(h % GROUP * ROWS, ROWS), :]

    copies = {}

    odd = (x + y + core) % 2
    second = (
        (x + 2 * odd, y + 2 * (1 - odd)),
        (x + 1 - odd, y + odd),
        (x + 3 * (1 - odd), y + 3 * odd),
        (x, y),
    )
    second = [(u % 4) * 4 + v % 4 for u, v in second]

    def step1(t, h, axis, d):
        return remote(
            send1.at[h, axis, d - 1],
            recv1[t % 2][h].at[pl.ds(axis * 24 + (d - 1) * 8, 8)],
            ss1.at[t % 2, h, axis, d - 1],
            rs1.at[t % 2, h, axis, d - 1],
            along[axis](d),
        )

    def step2(t, h, k):
        return remote(
            send2.at[h, k], recv2.at[t % 2, h, k], ss2.at[t % 2, h, k], rs2.at[t % 2, h, k], {"row": row, "col": second[k]}
        )

    def ship(t, h):
        def body(d, _):
            flipped = (x + y + core + d) % 2
            for axis in range(2):
                for e in range(2):
                    if axis == 0:
                        dest = wrap(x, d) * 4 + wrap(y, flipped + 2 * e)
                    else:
                        dest = wrap(x, 1 - flipped + 2 * e) * 4 + wrap(y, d)
                    for j in range(4):
                        send1[h, axis, d - 1, e * 4 + j] = part(h, tabs[PKEND, dest * 4 + j])
                step1(t, h, axis, d).start()
            return 0

        lax.fori_loop(1, 4, body, 0)

    def merge(t, h):
        for d in (1, 2, 3):
            for axis in range(2):
                step1(t, h, axis, d).wait()

        def summed(k, b):
            block = second[k] * 8 + b
            axis = odd if k in (0, 3) else 1 - odd
            total = part(h, tabs[DEND, block]).astype(F32)
            for d in (1, 2, 3):
                total = total + recv1[t % 2][h][idxs[axis * 3 + d - 1, block]].astype(F32)
            return total

        for k in range(4):

            def body(b, _):
                if k < 3:
                    send2[h, k, b] = summed(k, b).astype(BF16)
                else:
                    own[h, b] = summed(k, b)
                return 0

            lax.fori_loop(0, 8, body, 0, unroll=4)
            if k < 3:
                step2(t, h, k).start()

    def finish(t, h):
        for k in range(3):
            step2(t, h, k).wait()
        base = pl.multiple_of(row * 8, 8)
        queries = pl.ds(h * ROWS, ROWS)
        factor = coef[queries, :]
        for _ in range(t - 1):
            factor = factor * coef[queries, :]

        def body(b, _):
            total = own[h, b]
            for k in range(3):
                total = total + recv2[t % 2, h, k, b].astype(F32)
            if t == 0:
                score[b, queries, :] = total
            else:
                score[b, queries, :] = score[b, queries, :] + factor * total
            if t + 1 < TERMS:
                xg[t % 2][h][base + b] = total.astype(BF16)
            return 0

        lax.fori_loop(0, 8, body, 0, unroll=4)
        if t + 1 < TERMS:
            mine = xg[t % 2][h].at[pl.ds(base, 8)]
            for d in (1, 2, 3):
                c = remote(mine, mine, zss.at[t % 2, h, d - 1], zrs.at[t % 2, h, d - 1], up(d))
                c.start()
                copies[3, t, h, d] = c
            c = remote(mine, mine, css.at[t % 2, h, 0], crs.at[t % 2, h, 0], other)
            c.start()
            copies[4, t, h, 0] = c

    def hand_on(t, h):
        for d in (1, 3, 2):
            copies[3, t, h, d].wait()
            source = pl.multiple_of((wrap(z, 4 - d) * 2 + core) * 8, 8)
            part = xg[t % 2][h].at[pl.ds(source, 8)]
            c = remote(part, part, css.at[t % 2, h, d], crs.at[t % 2, h, d], other)
            c.start()
            copies[4, t, h, d] = c

    def gathered(t, h):
        for d in range(4):
            copies[4, t, h, d].wait()

    first_products()
    pl.semaphore_wait(barrier, len(peers))
    meta = []
    for half in range(2):
        for d in (1, 2, 3):
            at = half * 3 + d - 1
            meta.append(remote(tabv, metav.at[at], meta_ss.at[at], meta_rs.at[at], along[half](d)))
            meta[-1].start()
    for h in range(FIRST):
        ship(0, h)
    for c in meta:
        c.wait()
    lane1 = lax.broadcasted_iota(I32, (1, 128), 1)
    for axis in range(2):
        for d in (1, 2, 3):
            at = axis * 3 + d - 1
            place = metav[at, JIDX : JIDX + 1, :]
            away = ((lane1 >> 3) & 3) - y - odd if axis == 0 else (lane1 >> 5) - x - 1 + odd
            which = ((away + 8) & 3) >> 1
            idxv[at : at + 1, :] = jnp.where(place < 4, axis * 24 + (d - 1) * 8 + which * 4 + place, EMPTY)
    idxv[6:8, :] = jnp.zeros((2, 128), I32)
    to_scalar = pltpu.make_async_copy(idxv, idxs, copy_sem.at[1])
    to_scalar.start()
    to_scalar.wait()
    def compute(t, g):
        chunks = range(g * GROUP, (g + 1) * GROUP)
        if t:
            for h in chunks:
                gathered(t - 1, h)
            products(t, g)
        for h in chunks:
            if t or h >= FIRST:
                ship(t, h)

    steps = []
    for t in range(TERMS):
        for g in range(CHUNKS // GROUP):
            start = t + g * GROUP / CHUNKS * (1 if t else SPREAD)
            steps.append((start + NEXT - 1, 3, compute, t, g))
            for i in range(GROUP):
                at, h = start + i * LATER, g * GROUP + i
                steps += [(at + MERGE, 0, merge, t, h), (at + FINISH, 1, finish, t, h)]
                if t + 1 < TERMS:
                    steps.append((at + HAND_ON, 2, hand_on, t, h))
    steps.sort(key=lambda step: (round(step[0], 6), step[1]))
    for _, _, step, t, h in steps:
        step(t, h)
    for b in range(8):
        out[b * 128 : (b + 1) * 128, :] = jnp.transpose(score[b])


def shards(tiles, tile_row, tile_col, tile_count, query_ids, damping):
    vmem = pl.BlockSpec(memory_space=pltpu.VMEM)
    dma = pltpu.SemaphoreType.DMA
    return pl.pallas_call(
        kernel,
        out_shape=jax.ShapeDtypeStruct((1024, 128), F32),
        in_specs=[pl.BlockSpec(memory_space=pl.ANY), vmem, vmem, pl.BlockSpec(memory_space=pltpu.SMEM), vmem, vmem],
        out_specs=vmem,
        scratch_shapes=[
            pltpu.VMEM((SLOTS, 128, 128), BF16),
            pltpu.VMEM((SLOTS, 128, 128), BF16),
            pltpu.VMEM((8, 128), I32),
            pltpu.SMEM((8, 128), I32),
            pltpu.VMEM((6, 8, 128), I32),
            pltpu.VMEM((8, 128), I32),
            pltpu.SMEM((8, 128), I32),
            pltpu.VMEM((128, 128), I32),
            pltpu.VMEM((128, 128), F32),
            pltpu.VMEM((CHUNKS, 8, ROWS, 128), F32),
            pltpu.VMEM((8, 128, 128), F32),
            *[pltpu.VMEM((SLOTS + 1, GROUP * ROWS, 128), BF16) for _ in range(CHUNKS // GROUP)],
            *[pltpu.VMEM((64, ROWS, 128), BF16) for _ in range(2 * CHUNKS)],
            *[pltpu.VMEM((EMPTY + 1, ROWS, 128), BF16) for _ in range(2 * CHUNKS)],
            pltpu.VMEM((CHUNKS, 2, 3, 8, ROWS, 128), BF16),
            pltpu.VMEM((CHUNKS, 3, 8, ROWS, 128), BF16),
            pltpu.VMEM((2, CHUNKS, 3, 8, ROWS, 128), BF16),
            dma,
            dma((2,)),
            dma((6,)),
            dma((6,)),
            dma((2, CHUNKS, 2, 3)),
            dma((2, CHUNKS, 2, 3)),
            dma((2, CHUNKS, 3)),
            dma((2, CHUNKS, 3)),
            dma((2, CHUNKS, 3)),
            dma((2, CHUNKS, 3)),
            dma((2, CHUNKS, 4)),
            dma((2, CHUNKS, 4)),
        ],
        compiler_params=pltpu.CompilerParams(collective_id=0, has_side_effects=True, vmem_limit_bytes=60 * 2**20),
        name="katz",
    )(
        tiles.reshape(SLOTS, 128, 128),
        tile_row.reshape(1, SLOTS),
        tile_col.reshape(1, SLOTS),
        tile_count,
        query_ids.reshape(1, 128),
        damping.reshape(1, 128),
    )


def solution(mesh):
    in_specs = (
        P("row", "col", None, None, None),
        P("row", "col", None),
        P("row", "col", None),
        P("row", "col"),
        P(),
        P(),
    )
    out_specs = P(("row", "col"), None)
    return jax.shard_map(shards, mesh=mesh, in_specs=in_specs, out_specs=out_specs, check_vma=False)
```

```python
import functools

import jax
import jax.numpy as jnp
from jax import lax
from jax.experimental import pallas as pl
from jax.experimental.pallas import tpu as pltpu
from jax.sharding import PartitionSpec as P

TERMS = 4
PACK = 32
GROUP = 1
CHUNKS = 8
ROWS = 128 // CHUNKS
SLOTS = 128
NONE = 128
EMPTY = 48
EMPTY0 = 60
FIRST_UNROLL = 8
FIRST = 1
MERGE, FINISH, HAND_ON, NEXT = 0.26, 0.53, 0.8, 0.99
LATER, SPREAD = 0.0, 1.0
PERM, SCOL, KEEP, DEND, PKEND, SBASE, JIDX = range(7)
MESH = pl.DeviceIdType.MESH
BF16, F32, I32 = jnp.bfloat16, jnp.float32, jnp.int32


def down(row):
    return jnp.transpose(jnp.broadcast_to(row, (128, 128)))


def slot_tables(rows, cols, count, col_index):
    lane = lax.broadcasted_iota(I32, (128, 128), 1)
    sub = lax.broadcasted_iota(I32, (128, 128), 0)
    lane1 = lax.broadcasted_iota(I32, (1, 128), 1)
    key = jnp.where(lane1 < count, rows, 128)
    key_row = jnp.broadcast_to(key, (128, 128))
    key_col = down(key)

    def total(mask, value=1):
        return jnp.sum(jnp.where(mask, value, 0), axis=0, keepdims=True)

    earlier = (key_col == key_row) & (sub < lane)
    rank = total((key_col < key_row) | earlier)
    repeat = jnp.minimum(total(earlier), 1)
    place = down(rank) == lane
    perm = total(place, sub)
    scol = total(place, down(cols))
    keep = total(place, down(repeat))
    touched = total(key_col == lane) > 0
    upto = total(key_col <= lane)
    dend = jnp.where(touched, upto - 1, NONE)
    touched_col = down(touched.astype(I32)) > 0
    before = total(touched_col & ((sub >> 3) == (lane >> 3)) & (sub < lane))
    jidx = jnp.where(touched, before, 4)
    packed = touched_col & ((sub >> 3) == (lane >> 2)) & (down(before) == (lane & 3))
    ends = total(packed, down(upto))
    pkend = jnp.where(ends > 0, ends - 1, NONE)
    sbase = (((scol >> 3) * 16 + col_index) * 8 + (scol & 7)) * 128
    return jnp.concatenate([perm, scol, keep, dend, pkend, sbase, jidx, jidx], axis=0)


def kernel(short, tiles_hbm, trow, tcol, count, qids, damping, out, *scratch):
    scratch = list(scratch)
    take = lambda n: [scratch.pop(0) for _ in range(n)]
    raw, flip, tabv, tabs, metav, idxv, idxs, qmat, coef, own, score = take(11)
    run = take(CHUNKS // GROUP)
    xg = [take(CHUNKS) for _ in range(2)]
    recv1 = [take(CHUNKS) for _ in range(2)]
    send1, send2, recv2 = take(3)
    tile_sem, copy_sem, meta_ss, meta_rs, ss1, rs1, ss2, rs2, zss, zrs, css, crs = take(12)
    if short:
        run0, send0, recv0, idx0v, idx0s, place0, ss0, rs0 = take(8)

    row, col = lax.axis_index("row"), lax.axis_index("col")
    z, core = row // 2, row % 2
    x, y = col // 4, col % 4
    wrap = lambda v, d: (v + d) % 4
    along = (
        lambda d: {"row": row, "col": wrap(x, d) * 4 + y},
        lambda d: {"row": row, "col": x * 4 + wrap(y, d)},
    )
    across = lambda k: {"row": row, "col": wrap(x, k // 4) * 4 + wrap(y, k % 4)}
    near = [4, 8, 12, 1, 2, 3]
    greeted = range(1, 16) if short else near
    up = lambda d: {"row": wrap(z, d) * 2 + core, "col": col}
    other = {"row": z * 2 + 1 - core, "col": col}

    load = pltpu.make_async_copy(tiles_hbm, raw, tile_sem)
    load.start()
    barrier = pltpu.get_barrier_semaphore()
    peers = [across(k) for k in greeted] + [up(d) for d in (1, 2, 3)] + [other]
    for peer in peers:
        pl.semaphore_signal(barrier, inc=1, device_id=peer, device_id_type=MESH)

    def remote(src, dst, send_sem, recv_sem, peer):
        return pltpu.make_async_remote_copy(
            src_ref=src, dst_ref=dst, send_sem=send_sem, recv_sem=recv_sem, device_id=peer, device_id_type=MESH
        )

    tabv[...] = slot_tables(trow[...], tcol[...], count[0, 0], col)
    to_scalar = pltpu.make_async_copy(tabv, tabs, copy_sem.at[0])
    to_scalar.start()
    lane = lax.broadcasted_iota(I32, (128, 128), 1)
    if short:
        sub = lax.broadcasted_iota(I32, (128, 128), 0)
        queries = qids[...]
        owner = (queries >> 10) & 15
        owner_col = down(owner)
        rank = jnp.sum(jnp.where((owner_col == owner) & (sub < lane), 1, 0), axis=0, keepdims=True)
        packed = (owner_col == col) & (down(rank) == lane)
        ids = jnp.sum(jnp.where(packed, down(queries) + 1, 0), axis=0, keepdims=True)
        qmat[...] = down(jnp.where(ids > 0, ids - 1, -(2**20))) - lane
        source = ((x - (owner >> 2) + 4) & 3) * 4 + ((y - (owner & 3) + 4) & 3)
        target = down(source * PACK + rank)
        for m in range(4):
            place0[:, m * 128 : (m + 1) * 128] = (target == lane + m * 128).astype(F32).astype(BF16)
        run0[NONE] = jnp.zeros((PACK, 128), BF16)
        recv0[EMPTY0] = jnp.zeros((PACK, 128), BF16)
    else:
        qmat[...] = down(qids[...]) - lane
    coef[...] = down(damping[...])
    for g in range(CHUNKS // GROUP):
        run[g][NONE] = jnp.zeros((GROUP * ROWS, 128), BF16)
    for h in range(CHUNKS):
        for parity in range(2):
            recv1[parity][h][EMPTY] = jnp.zeros((ROWS, 128), BF16)
    to_scalar.wait()
    load.wait()

    def first_products():
        height = PACK if short else 128

        def body(step, total):
            for u in range(FIRST_UNROLL):
                s = step * FIRST_UNROLL + u
                tile = raw[tabs[PERM, s]]
                hot = (qmat[0:height, :] == tabs[SBASE, s]).astype(BF16)
                prod = lax.dot_general(hot, tile, (((1,), (1,)), ((), ())), preferred_element_type=F32)
                total = jnp.where(tabs[KEEP, s] > 0, prod + total, prod)
                rounded = total.astype(BF16)
                if short:
                    run0[s] = rounded
                else:
                    for g in range(CHUNKS // GROUP):
                        run[g][s] = rounded[g * GROUP * ROWS : (g + 1) * GROUP * ROWS]
                flip[s] = jnp.transpose(tile)
            return total

        lax.fori_loop(0, SLOTS // FIRST_UNROLL, body, jnp.zeros((height, 128), F32))

    unroll = 64 if short else 2

    def products(t, g):
        sources = [xg[(t - 1) % 2][g * GROUP + i] for i in range(GROUP)]

        def body(step, total):
            for u in range(unroll):
                s = step * unroll + u
                left = jnp.concatenate([source[tabs[SCOL, s]] for source in sources], axis=0)
                prod = jnp.dot(left, flip[s], preferred_element_type=F32)
                total = jnp.where(tabs[KEEP, s] > 0, prod + total, prod)
                run[g][s] = total.astype(BF16)
            return total

        lax.fori_loop(0, SLOTS // unroll, body, jnp.zeros((GROUP * ROWS, 128), F32))

    def part(h, index):
        return run[h // GROUP][index, pl.ds(h % GROUP * ROWS, ROWS), :]

    copies = {}

    odd = (x + y + core) % 2
    second = (
        (x + 2 * odd, y + 2 * (1 - odd)),
        (x + 1 - odd, y + odd),
        (x + 3 * (1 - odd), y + 3 * odd),
        (x, y),
    )
    second = [(u % 4) * 4 + v % 4 for u, v in second]

    def step1(t, h, axis, d):
        return remote(
            send1.at[h, axis, d - 1],
            recv1[t % 2][h].at[pl.ds(axis * 24 + (d - 1) * 8, 8)],
            ss1.at[t % 2, h, axis, d - 1],
            rs1.at[t % 2, h, axis, d - 1],
            along[axis](d),
        )

    def step2(t, h, k):
        return remote(
            send2.at[h, k], recv2.at[t % 2, h, k], ss2.at[t % 2, h, k], rs2.at[t % 2, h, k], {"row": row, "col": second[k]}
        )

    def ship(t, h):
        def body(d, _):
            flipped = (x + y + core + d) % 2
            for axis in range(2):
                for e in range(2):
                    if axis == 0:
                        dest = wrap(x, d) * 4 + wrap(y, flipped + 2 * e)
                    else:
                        dest = wrap(x, 1 - flipped + 2 * e) * 4 + wrap(y, d)
                    for j in range(4):
                        send1[h, axis, d - 1, e * 4 + j] = part(h, tabs[PKEND, dest * 4 + j])
                step1(t, h, axis, d).start()
            return 0

        lax.fori_loop(1, 4, body, 0)

    def merge(t, h):
        for d in (1, 2, 3):
            for axis in range(2):
                step1(t, h, axis, d).wait()

        def summed(k, b):
            block = second[k] * 8 + b
            axis = odd if k in (0, 3) else 1 - odd
            total = part(h, tabs[DEND, block]).astype(F32)
            for d in (1, 2, 3):
                total = total + recv1[t % 2][h][idxs[axis * 3 + d - 1, block]].astype(F32)
            return total

        for k in range(4):

            def body(b, _):
                if k < 3:
                    send2[h, k, b] = summed(k, b).astype(BF16)
                else:
                    own[h, b] = summed(k, b)
                return 0

            lax.fori_loop(0, 8, body, 0, unroll=4 if short else 1)
            if k < 3:
                step2(t, h, k).start()

    def finish(t, h):
        for k in range(3):
            step2(t, h, k).wait()
        base = pl.multiple_of(row * 8, 8)
        queries = pl.ds(h * ROWS, ROWS)
        factor = coef[queries, :]
        for _ in range(t - 1):
            factor = factor * coef[queries, :]

        def body(b, _):
            total = own[h, b]
            for k in range(3):
                total = total + recv2[t % 2, h, k, b].astype(F32)
            if t == 0:
                score[b, queries, :] = total
            else:
                score[b, queries, :] = score[b, queries, :] + factor * total
            if t + 1 < TERMS:
                xg[t % 2][h][base + b] = total.astype(BF16)
            return 0

        lax.fori_loop(0, 8, body, 0, unroll=4 if short else 1)
        if t + 1 < TERMS:
            spread(t, h)

    def spread(t, h):
        mine = xg[t % 2][h].at[pl.ds(pl.multiple_of(row * 8, 8), 8)]
        for d in (1, 2, 3):
            c = remote(mine, mine, zss.at[t % 2, h, d - 1], zrs.at[t % 2, h, d - 1], up(d))
            c.start()
            copies[3, t, h, d] = c
        c = remote(mine, mine, css.at[t % 2, h, 0], crs.at[t % 2, h, 0], other)
        c.start()
        copies[4, t, h, 0] = c

    def step0(k):
        return remote(
            send0.at[k - 1], recv0.at[pl.ds((k - 1) * 4, 4)], ss0.at[k - 1], rs0.at[k - 1], across(k)
        )

    def ship_short():
        def body(k, _):
            dest = wrap(x, k // 4) * 4 + wrap(y, k % 4)
            for j in range(4):
                send0[k - 1, j] = run0[tabs[PKEND, dest * 4 + j]]
            step0(k).start()
            return 0

        lax.fori_loop(1, 16, body, 0)

    def finish_short():
        for k in range(1, 16):
            step0(k).wait()
        base = pl.multiple_of(row * 8, 8)

        def body(b, _):
            block = col * 8 + b
            parts = [run0[tabs[DEND, block]]] + [recv0[idx0s[k - 1, block]] for k in range(1, 16)]
            total = jnp.dot(place0[...], jnp.concatenate(parts, axis=0), preferred_element_type=F32)
            score[b] = total
            rounded = total.astype(BF16)
            for h in range(CHUNKS):
                xg[0][h][base + b] = rounded[h * ROWS : (h + 1) * ROWS]
            return 0

        lax.fori_loop(0, 8, body, 0)

    def hand_on(t, h):
        for d in (1, 3, 2):
            copies[3, t, h, d].wait()
            source = pl.multiple_of((wrap(z, 4 - d) * 2 + core) * 8, 8)
            part = xg[t % 2][h].at[pl.ds(source, 8)]
            c = remote(part, part, css.at[t % 2, h, d], crs.at[t % 2, h, d], other)
            c.start()
            copies[4, t, h, d] = c

    def gathered(t, h):
        for d in range(4):
            copies[4, t, h, d].wait()

    first_products()
    pl.semaphore_wait(barrier, len(peers))
    meta = []
    for at, k in enumerate(greeted):
        meta.append(remote(tabv, metav.at[at], meta_ss.at[at], meta_rs.at[at], across(k)))
        meta[-1].start()
    if short:
        ship_short()
    else:
        for h in range(FIRST):
            ship(0, h)
    for c in meta:
        c.wait()
    lane1 = lax.broadcasted_iota(I32, (1, 128), 1)
    for axis in range(2):
        for d in (1, 2, 3):
            at = axis * 3 + d - 1
            place = metav[near[at] - 1 if short else at, JIDX : JIDX + 1, :]
            away = ((lane1 >> 3) & 3) - y - odd if axis == 0 else (lane1 >> 5) - x - 1 + odd
            which = ((away + 8) & 3) >> 1
            idxv[at : at + 1, :] = jnp.where(place < 4, axis * 24 + (d - 1) * 8 + which * 4 + place, EMPTY)
    idxv[6:8, :] = jnp.zeros((2, 128), I32)
    to_scalar = pltpu.make_async_copy(idxv, idxs, copy_sem.at[1])
    to_scalar.start()
    if short:
        for k in range(1, 16):
            place = metav[k - 1, JIDX : JIDX + 1, :]
            idx0v[k - 1 : k, :] = jnp.where(place < 4, (k - 1) * 4 + place, EMPTY0)
        idx0v[15:16, :] = jnp.zeros((1, 128), I32)
        to_scalar0 = pltpu.make_async_copy(idx0v, idx0s, copy_sem.at[2])
        to_scalar0.start()
        to_scalar0.wait()
    to_scalar.wait()
    if short:
        finish_short()
        for h in range(CHUNKS):
            spread(0, h)
    def compute(t, g):
        chunks = range(g * GROUP, (g + 1) * GROUP)
        if t:
            for h in chunks:
                gathered(t - 1, h)
            products(t, g)
        for h in chunks:
            if t or h >= FIRST:
                ship(t, h)

    steps = []
    for t in range(TERMS):
        for g in range(CHUNKS // GROUP):
            start = t + g * GROUP / CHUNKS * (1 if t else SPREAD)
            if t or not short:
                steps.append((start + NEXT - 1, 3, compute, t, g))
            for i in range(GROUP):
                at, h = start + i * LATER, g * GROUP + i
                if t or not short:
                    steps += [(at + MERGE, 0, merge, t, h), (at + FINISH, 1, finish, t, h)]
                if t + 1 < TERMS:
                    steps.append((at + HAND_ON, 2, hand_on, t, h))
    steps.sort(key=lambda step: (round(step[0], 6), step[1]))
    for _, _, step, t, h in steps:
        step(t, h)
    for b in range(8):
        out[b * 128 : (b + 1) * 128, :] = jnp.transpose(score[b])


def short_scratch():
    return (
        pltpu.VMEM((SLOTS + 1, PACK, 128), BF16),
        pltpu.VMEM((15, 4, PACK, 128), BF16),
        pltpu.VMEM((EMPTY0 + 1, PACK, 128), BF16),
        pltpu.VMEM((16, 128), I32),
        pltpu.SMEM((16, 128), I32),
        pltpu.VMEM((128, 512), BF16),
        pltpu.SemaphoreType.DMA((15,)),
        pltpu.SemaphoreType.DMA((15,)),
    )


def call(short, tiles, tile_row, tile_col, tile_count, query_ids, damping):
    vmem = pl.BlockSpec(memory_space=pltpu.VMEM)
    dma = pltpu.SemaphoreType.DMA
    return pl.pallas_call(
        functools.partial(kernel, short),
        out_shape=jax.ShapeDtypeStruct((1024, 128), F32),
        in_specs=[pl.BlockSpec(memory_space=pl.ANY), vmem, vmem, pl.BlockSpec(memory_space=pltpu.SMEM), vmem, vmem],
        out_specs=vmem,
        scratch_shapes=[
            pltpu.VMEM((SLOTS, 128, 128), BF16),
            pltpu.VMEM((SLOTS, 128, 128), BF16),
            pltpu.VMEM((8, 128), I32),
            pltpu.SMEM((8, 128), I32),
            pltpu.VMEM((15 if short else 6, 8, 128), I32),
            pltpu.VMEM((8, 128), I32),
            pltpu.SMEM((8, 128), I32),
            pltpu.VMEM((128, 128), I32),
            pltpu.VMEM((128, 128), F32),
            pltpu.VMEM((CHUNKS, 8, ROWS, 128), F32),
            pltpu.VMEM((8, 128, 128), F32),
            *[pltpu.VMEM((SLOTS + 1, GROUP * ROWS, 128), BF16) for _ in range(CHUNKS // GROUP)],
            *[pltpu.VMEM((64, ROWS, 128), BF16) for _ in range(2 * CHUNKS)],
            *[pltpu.VMEM((EMPTY + 1, ROWS, 128), BF16) for _ in range(2 * CHUNKS)],
            pltpu.VMEM((CHUNKS, 2, 3, 8, ROWS, 128), BF16),
            pltpu.VMEM((CHUNKS, 3, 8, ROWS, 128), BF16),
            pltpu.VMEM((2, CHUNKS, 3, 8, ROWS, 128), BF16),
            dma,
            dma((3,)),
            dma((15,)),
            dma((15,)),
            dma((2, CHUNKS, 2, 3)),
            dma((2, CHUNKS, 2, 3)),
            dma((2, CHUNKS, 3)),
            dma((2, CHUNKS, 3)),
            dma((2, CHUNKS, 3)),
            dma((2, CHUNKS, 3)),
            dma((2, CHUNKS, 4)),
            dma((2, CHUNKS, 4)),
            *(short_scratch() if short else ()),
        ],
        compiler_params=pltpu.CompilerParams(collective_id=int(short), has_side_effects=True, vmem_limit_bytes=60 * 2**20),
        name="katz_short" if short else "katz",
    )(
        tiles.reshape(SLOTS, 128, 128),
        tile_row.reshape(1, SLOTS),
        tile_col.reshape(1, SLOTS),
        tile_count,
        query_ids.reshape(1, 128),
        damping.reshape(1, 128),
    )


def shards(tiles, tile_row, tile_col, tile_count, query_ids, damping):
    owner = (query_ids >> 10) & 15
    held = jnp.sum((owner[:, None] == jnp.arange(16, dtype=I32)[None, :]).astype(I32), axis=0)
    args = (tiles, tile_row, tile_col, tile_count, query_ids, damping)
    return lax.cond(jnp.max(held) <= PACK, functools.partial(call, True), functools.partial(call, False), *args)


def solution(mesh):
    in_specs = (
        P("row", "col", None, None, None),
        P("row", "col", None),
        P("row", "col", None),
        P("row", "col"),
        P(),
        P(),
    )
    out_specs = P(("row", "col"), None)
    return jax.shard_map(shards, mesh=mesh, in_specs=in_specs, out_specs=out_specs, check_vma=False)
```
